16 devices in a mesh: dp: 4 (over z, y), sp: 4 (over x, core).
Axes of the slice: x: 2, y: 2, z: 2, core: 2. Of those that a mesh axis runs over, the one named last changes fastest.
Arguments:
- x_tokens: bfloat16 [64, 512, 4096], P('dp', 'sp'), parts along dimension 0
- dy_tokens: bfloat16 [64, 512, 4096], P('dp', 'sp'), parts along dimension 0
- positions: int32 [64, 512], P('dp', 'sp'), parts along dimension 0
- ln_gain: float32 [4096], replicated
- ln_bias: float32 [4096], replicated
- w_q: bfloat16 [4096, 4096], replicated
- w_k: bfloat16 [4096, 1024], replicated
- w_v: bfloat16 [4096, 1024], replicated
- w_o: bfloat16 [4096, 4096], replicated
Outputs:
- output 1: bfloat16 [64, 512, 4096], P('dp', 'sp'), parts along dimension 0
- output 2: bfloat16 [64, 512, 4096], P('dp', 'sp'), parts along dimension 0
- output 3: float32 [65536], P(('dp', 'sp')), parts along dimension 0
- output 4: float32 [65536], P(('dp', 'sp')), parts along dimension 0
There are 4 independent parts. The reference program is written for one: setup_inputs(seed, part) draws one part's arguments, and reference() takes and returns one part's arrays. A program takes and returns all parts, laid end to end along the dimension named above; an argument that names none is the same for every part.
All inputs are finite; a program needn't handle non-finite values.
Results may differ from the reference program's by a relative error of at most 0.0150938.
Values are sent between devices in bfloat16 or wider.
A program may use at most 1 GiB of HBM per device.

```python
import math
import jax
import jax.numpy as jnp
from jax import lax

BATCH_SIZE = 16
SEQ_PER_DEV = 128
SEQ_SHARDS = 4
MODEL_DIM = 4096
Q_HEADS = 32
KV_HEADS = 8
HEAD_DIM = 128
SEQ_LEN = SEQ_PER_DEV * SEQ_SHARDS
GROUP_SIZE = Q_HEADS // KV_HEADS
ROT_HALF = HEAD_DIM // 4
QUERY_BLOCK = min(SEQ_LEN, 64)
ROPE_BASE = 10000.0
LN_EPS = 1e-5


def setup_inputs(seed: int = 0, part: int = 0) -> dict:
    part_keys = jax.random.split(jax.random.fold_in(jax.random.key(seed), part), 3)
    shared_keys = jax.random.split(jax.random.key(seed + 1), 6)
    tok_shape = (BATCH_SIZE, SEQ_LEN, MODEL_DIM)
    x_tokens = jax.random.normal(part_keys[0], tok_shape, jnp.float32).astype(jnp.bfloat16)
    dy_tokens = jax.random.normal(part_keys[1], tok_shape, jnp.float32).astype(jnp.bfloat16)
    pos_gaps = jax.random.randint(part_keys[2], (BATCH_SIZE, SEQ_LEN), 1, 4, dtype=jnp.int32)
    positions = (jnp.cumsum(pos_gaps, axis=1) - pos_gaps[:, :1]).astype(jnp.int32)
    score_gain = math.log(SEQ_LEN / 16.0) ** 0.25
    qk_scale = score_gain * MODEL_DIM ** -0.5
    w_q = (jax.random.normal(shared_keys[0], (MODEL_DIM, Q_HEADS * HEAD_DIM), jnp.float32) * qk_scale).astype(jnp.bfloat16)
    w_k = (jax.random.normal(shared_keys[1], (MODEL_DIM, KV_HEADS * HEAD_DIM), jnp.float32) * qk_scale).astype(jnp.bfloat16)
    w_v = (jax.random.normal(shared_keys[2], (MODEL_DIM, KV_HEADS * HEAD_DIM), jnp.float32) * MODEL_DIM ** -0.5).astype(jnp.bfloat16)
    w_o = (jax.random.normal(shared_keys[3], (Q_HEADS * HEAD_DIM, MODEL_DIM), jnp.float32) * (3.0 * (Q_HEADS * HEAD_DIM) ** -0.5)).astype(jnp.bfloat16)
    ln_gain = 0.3 * jax.random.normal(shared_keys[4], (MODEL_DIM,), jnp.float32)
    ln_bias = 0.3 * jax.random.normal(shared_keys[5], (MODEL_DIM,), jnp.float32)
    return {'x_tokens': x_tokens, 'dy_tokens': dy_tokens, 'positions': positions, 'ln_gain': ln_gain, 'ln_bias': ln_bias, 'w_q': w_q, 'w_k': w_k, 'w_v': w_v, 'w_o': w_o}


def rope_tables(positions):
    inv_freq = ROPE_BASE ** (-jnp.arange(ROT_HALF, dtype=jnp.float32) / ROT_HALF)
    angles = positions.astype(jnp.float32)[:, :, None] * inv_freq
    return jnp.cos(angles)[:, :, None, :], jnp.sin(angles)[:, :, None, :]


def rotate(tensor, cos_table, sin_table):
    lower_half = tensor[..., :ROT_HALF]
    upper_half = tensor[..., ROT_HALF:2 * ROT_HALF]
    return jnp.concatenate([lower_half * cos_table - upper_half * sin_table, upper_half * cos_table + lower_half * sin_table, tensor[..., 2 * ROT_HALF:]], axis=-1)


def causal_attention(queries, key_rows, value_rows):
    n_blocks = SEQ_LEN // QUERY_BLOCK
    q_grouped = queries.astype(jnp.float32).reshape(BATCH_SIZE, n_blocks, QUERY_BLOCK, KV_HEADS, GROUP_SIZE, HEAD_DIM)
    q_blocks = jnp.moveaxis(q_grouped, 1, 0)
    key_float = key_rows.astype(jnp.float32)
    value_float = value_rows.astype(jnp.float32)
    key_pos = jnp.arange(SEQ_LEN)
    score_scale = HEAD_DIM ** -0.5

    def one_block(block_args):
        q_piece, block_idx = block_args
        scores = jnp.einsum('bqkgd,bskd->bkgqs', q_piece, key_float) * score_scale
        q_pos = block_idx * QUERY_BLOCK + jnp.arange(QUERY_BLOCK)
        scores = jnp.where(key_pos[None, :] <= q_pos[:, None], scores, -1e30)
        attn_prob = jax.nn.softmax(scores, axis=-1)
        return jnp.einsum('bkgqs,bskd->bqkgd', attn_prob, value_float).astype(jnp.bfloat16)

    block_outs = lax.map(jax.checkpoint(one_block), (q_blocks, jnp.arange(n_blocks)))
    return jnp.moveaxis(block_outs, 0, 1).reshape(BATCH_SIZE, SEQ_LEN, Q_HEADS, HEAD_DIM)


def block_forward(x_tokens, gain_rows, bias_rows, positions, w_q, w_k, w_v, w_o):
    x_float = x_tokens.astype(jnp.float32)
    centered = x_float - jnp.mean(x_float, axis=-1, keepdims=True)
    x_hat = centered * lax.rsqrt(jnp.mean(centered * centered, axis=-1, keepdims=True) + LN_EPS)
    x_view = x_hat.reshape(BATCH_SIZE, SEQ_SHARDS, SEQ_PER_DEV, MODEL_DIM)
    normed = (x_view * (1.0 + gain_rows[None, :, None, :]) + bias_rows[None, :, None, :]).astype(jnp.bfloat16)
    normed_flat = normed.reshape(BATCH_SIZE * SEQ_LEN, MODEL_DIM)
    cos_table, sin_table = rope_tables(positions)
    q_lin = jnp.dot(normed_flat, w_q, preferred_element_type=jnp.float32).reshape(BATCH_SIZE, SEQ_LEN, Q_HEADS, HEAD_DIM)
    k_lin = jnp.dot(normed_flat, w_k, preferred_element_type=jnp.float32).reshape(BATCH_SIZE, SEQ_LEN, KV_HEADS, HEAD_DIM)
    v_lin = jnp.dot(normed_flat, w_v, preferred_element_type=jnp.float32).reshape(BATCH_SIZE, SEQ_LEN, KV_HEADS, HEAD_DIM)
    queries = rotate(q_lin, cos_table, sin_table).astype(jnp.bfloat16)
    key_rows = rotate(k_lin, cos_table, sin_table).astype(jnp.bfloat16)
    value_rows = v_lin.astype(jnp.bfloat16)
    attn_out = causal_attention(queries, key_rows, value_rows).reshape(BATCH_SIZE * SEQ_LEN, Q_HEADS * HEAD_DIM)
    out_proj = jnp.dot(attn_out, w_o, preferred_element_type=jnp.float32).reshape(BATCH_SIZE, SEQ_LEN, MODEL_DIM)
    return (x_float + out_proj).astype(jnp.bfloat16)


def reference(x_tokens, dy_tokens, positions, ln_gain, ln_bias, w_q, w_k, w_v, w_o):
    gain_rows = jnp.broadcast_to(ln_gain, (SEQ_SHARDS, MODEL_DIM))
    bias_rows = jnp.broadcast_to(ln_bias, (SEQ_SHARDS, MODEL_DIM))

    def block_fn(x_in, gain_in, bias_in):
        return block_forward(x_in, gain_in, bias_in, positions, w_q, w_k, w_v, w_o)

    out_tokens, pullback = jax.vjp(block_fn, x_tokens, gain_rows, bias_rows)
    dx_tokens, d_gain, d_bias = pullback(dy_tokens)
    return out_tokens, dx_tokens, d_gain.reshape(-1), d_bias.reshape(-1)
```

```python
import math
import jax
import jax.numpy as jnp
from jax import lax
from jax.experimental import pallas as pl
from jax.experimental.pallas import tpu as pltpu
from jax.sharding import PartitionSpec as P

HEAD_DIM = 128
ROT_HALF = HEAD_DIM // 4
ROPE_BASE = 10000.0
LN_EPS = 1e-5
NEG_BIG = -1e30
CHUNKS = 4
HALVES = 2
SCALE = HEAD_DIM ** -0.5
EXP_SCALE = SCALE * math.log2(math.e)
KV_WIDTH = 2 * HEAD_DIM


PAIRS_A = [(0, 1), (2, 3)]
PAIRS_B = [(0, 2), (1, 3)]
PAIRS_C = [(2, 3), (3, 2)]


def reverse(pairs):
    return [(target, source) for source, target in pairs]


def rope_tables(positions):
    inv_freq = ROPE_BASE ** (-jnp.arange(ROT_HALF, dtype=jnp.float32) / ROT_HALF)
    angles = positions.astype(jnp.float32)[:, None] * inv_freq
    cos, sin = jnp.cos(angles), jnp.sin(angles)
    zero = jnp.zeros_like(sin)
    one = jnp.ones_like(sin)
    return jnp.concatenate([cos, cos, one, one, -sin, zero, zero, zero, zero, sin, zero, zero], axis=1)


def rotate(tensor, table, sign):
    cos = table[:, :HEAD_DIM]
    sin_low = table[:, HEAD_DIM:2 * HEAD_DIM]
    sin_high = table[:, 2 * HEAD_DIM:]
    turned = pltpu.roll(tensor, HEAD_DIM - ROT_HALF, 1) * sin_low + pltpu.roll(tensor, ROT_HALF, 1) * sin_high
    return tensor * cos + turned if sign > 0 else tensor * cos - turned


def pack_kernel(table_ref, lin_ref, *rest):
    out_ref = rest[-1]
    table = table_ref[...]
    for head in range(lin_ref.shape[1] // KV_WIDTH):
        k_cols = slice(head * KV_WIDTH, head * KV_WIDTH + HEAD_DIM)
        v_cols = slice(head * KV_WIDTH + HEAD_DIM, (head + 1) * KV_WIDTH)
        out_ref[:, k_cols] = rotate(lin_ref[:, k_cols], table, 1).astype(jnp.bfloat16)
        out_ref[:, v_cols] = lin_ref[:, v_cols].astype(jnp.bfloat16)


def join_kernel(wk_ref, wv_ref, out_ref):
    for head in range(wk_ref.shape[1] // HEAD_DIM):
        cols = slice(head * HEAD_DIM, (head + 1) * HEAD_DIM)
        out_ref[:, head * KV_WIDTH:head * KV_WIDTH + HEAD_DIM] = wk_ref[:, cols]
        out_ref[:, head * KV_WIDTH + HEAD_DIM:(head + 1) * KV_WIDTH] = wv_ref[:, cols]


def add_kernel(left_ref, right_ref, out_ref):
    out_ref[...] = left_ref[...] + right_ref[...]


def finish_kernel(table_ref, own_ref, a_ref, b_ref, *rest):
    out_ref = rest[-1]
    table = table_ref[...]
    for head in range(own_ref.shape[1] // KV_WIDTH):
        k_cols = slice(head * KV_WIDTH, head * KV_WIDTH + HEAD_DIM)
        v_cols = slice(head * KV_WIDTH + HEAD_DIM, (head + 1) * KV_WIDTH)
        d_key = (own_ref[:, k_cols] + a_ref[:, k_cols] + b_ref[:, k_cols]).astype(jnp.bfloat16).astype(jnp.float32)
        d_val = own_ref[:, v_cols] + a_ref[:, v_cols] + b_ref[:, v_cols]
        out_ref[:, k_cols] = rotate(d_key, table, -1).astype(jnp.bfloat16)
        out_ref[:, v_cols] = d_val.astype(jnp.bfloat16)


def dot(lhs, rhs, contract):
    return lax.dot_general(lhs, rhs, (contract, ((), ())), preferred_element_type=jnp.float32)


def attend_kernel(flags_ref, table_ref, q_ref, do_ref, own_ref, a_ref, b_ref, c_ref, *rest):
    o_ref, dq_ref, d_own_ref, d_a_ref, d_b_ref, d_c_ref = rest[-6:]
    seq = q_ref.shape[0]
    table = table_ref[...]
    kv_refs = (own_ref, a_ref, b_ref, c_ref)
    d_refs = (d_own_ref, d_a_ref, d_b_ref, d_c_ref)
    keys = jnp.concatenate([ref[:, :HEAD_DIM] for ref in kv_refs], axis=0)
    values = jnp.concatenate([ref[:, HEAD_DIM:] for ref in kv_refs], axis=0)
    keys_t = keys.T
    values_t = values.T
    off_a = (1 - flags_ref[0]).astype(jnp.float32) * 1e30
    off_bc = (1 - flags_ref[1]).astype(jnp.float32) * 1e30
    offsets = (None, off_a, off_bc, off_bc)
    n_heads = q_ref.shape[1] // HEAD_DIM
    step = 2
    d_keys = None
    d_values = None
    key_pos = lax.broadcasted_iota(jnp.int32, (seq, step * seq), 0)
    query_pos = lax.broadcasted_iota(jnp.int32, (seq, step * seq), 1) % seq
    visible = key_pos <= query_pos
    for first in range(0, n_heads, step):
        cols = [slice(h * HEAD_DIM, (h + 1) * HEAD_DIM) for h in range(first, first + step)]
        q = jnp.concatenate([rotate(q_ref[:, col], table, 1).astype(jnp.bfloat16) for col in cols], axis=0)
        d_out = jnp.concatenate([do_ref[:, col] for col in cols], axis=0)
        scores = dot(keys, q, ((1,), (1,)))
        parts = [scores[j * seq:(j + 1) * seq] for j in range(4)]
        parts[0] = jnp.where(visible, parts[0], NEG_BIG)
        peak = jnp.max(parts[0], axis=0, keepdims=True)
        for part, off in zip(parts[1:], offsets[1:]):
            peak = jnp.maximum(peak, jnp.max(part, axis=0, keepdims=True) - off)
        peak = peak * EXP_SCALE
        weights = [jnp.exp2(parts[0] * EXP_SCALE - peak)]
        for part, off in zip(parts[1:], offsets[1:]):
            weights.append(jnp.exp2(part * EXP_SCALE - (peak + off)))
        total = sum(jnp.sum(w, axis=0, keepdims=True) for w in weights)
        prob = jnp.concatenate(weights, axis=0) * (1.0 / total)
        prob_b = prob.astype(jnp.bfloat16)
        d_prob = dot(values, d_out, ((1,), (1,)))
        delta = jnp.sum(prob * d_prob, axis=0, keepdims=True)
        d_scores = (prob * (d_prob - delta)).astype(jnp.bfloat16)
        out_t = dot(values_t, prob_b, ((1,), (0,))).astype(jnp.bfloat16)
        dq_t = dot(keys_t, d_scores, ((1,), (0,))) * SCALE
        for i, col in enumerate(cols):
            lanes = slice(i * seq, (i + 1) * seq)
            o_ref[:, col] = out_t[:, lanes].T
            dq = dq_t[:, lanes].T.astype(jnp.bfloat16).astype(jnp.float32)
            dq_ref[:, col] = rotate(dq, table, -1).astype(jnp.bfloat16)
        d_k = dot(d_scores, q, ((1,), (0,)))
        d_v = dot(prob_b, d_out, ((1,), (0,)))
        d_keys = d_k if d_keys is None else d_keys + d_k
        d_values = d_v if d_values is None else d_values + d_v
    d_keys = d_keys * SCALE
    for j, ref in enumerate(d_refs):
        ref[:, :HEAD_DIM] = d_keys[j * seq:(j + 1) * seq]
        ref[:, HEAD_DIM:] = d_values[j * seq:(j + 1) * seq]


def solution(mesh):
    def block_step(x_tokens, dy_tokens, positions, ln_gain, ln_bias, w_q, w_k, w_v, w_o):
        n_batch, seq, model_dim = x_tokens.shape
        n_kv = w_k.shape[1] // HEAD_DIM
        group = w_q.shape[1] // w_k.shape[1]
        q_width = group * HEAD_DIM
        kv_cols = n_kv * KV_WIDTH
        tokens = n_batch * seq
        rows_b = n_batch // CHUNKS
        chunk_rows = rows_b * seq
        x_flat = x_tokens.reshape(tokens, model_dim)
        dy_flat = dy_tokens.reshape(tokens, model_dim)
        rank = lax.axis_index('sp')
        flags = jnp.stack([rank % 2, rank // 2]).astype(jnp.int32)

        x_float = x_flat.astype(jnp.float32)
        centered = x_float - jnp.mean(x_float, axis=-1, keepdims=True)
        inv_std = lax.rsqrt(jnp.mean(centered * centered, axis=-1, keepdims=True) + LN_EPS)
        x_hat = centered * inv_std
        normed = (x_hat * (1.0 + ln_gain) + ln_bias).astype(jnp.bfloat16)
        table = rope_tables(positions.reshape(tokens))
        w_rows = math.gcd(model_dim, 512)
        w_kv = pl.pallas_call(
            join_kernel, grid=(model_dim // w_rows,), in_specs=[pl.BlockSpec((w_rows, kv_cols // 2), lambda i: (i, 0))] * 2,
            out_specs=pl.BlockSpec((w_rows, kv_cols), lambda i: (i, 0)), out_shape=jax.ShapeDtypeStruct((model_dim, kv_cols), jnp.bfloat16), name='join_kv',
            cost_estimate=pl.CostEstimate(flops=model_dim * kv_cols * 300, bytes_accessed=model_dim * kv_cols * 4, transcendentals=0),
        )(w_k, w_v)
        kv_lin = jnp.dot(normed, w_kv, preferred_element_type=jnp.float32)

        table_width = 3 * HEAD_DIM

        def row_spec(width, base=0):
            return pl.BlockSpec((seq, width), lambda b: (b + base, 0))

        def pack(chunk, before):
            base = chunk * rows_b
            return pl.pallas_call(
                pack_kernel, grid=(rows_b,),
                in_specs=[row_spec(table_width, base), row_spec(kv_cols, base)] + [pl.BlockSpec(memory_space=pl.ANY)] * len(before), out_specs=row_spec(kv_cols),
                out_shape=jax.ShapeDtypeStruct((chunk_rows, kv_cols), jnp.bfloat16), name='pack_kv',
                cost_estimate=pl.CostEstimate(flops=chunk_rows * kv_cols * 300, bytes_accessed=chunk_rows * kv_cols * 6, transcendentals=0),
            )(table, kv_lin, *before)

        def send(value, pairs):
            return lax.ppermute(value, 'sp', pairs)

        own = []
        for c in range(CHUNKS):
            own.append(pack(c, own[-1:]))
        from_b = [send(own[c], PAIRS_B) for c in range(CHUNKS)]
        from_a = [send(own[c], PAIRS_A) for c in range(CHUNKS)]
        from_c = [send(from_b[c], PAIRS_C) for c in range(CHUNKS)]

        half_rows = tokens // HALVES
        q_half, da_half = [], []
        for i in range(HALVES):
            rows = slice(i * half_rows, (i + 1) * half_rows)
            q_half.append(jnp.dot(normed[rows], w_q, preferred_element_type=jnp.float32))
            da_half.append(jnp.einsum('td,fd->tf', dy_flat[rows], w_o, preferred_element_type=jnp.float32).astype(jnp.bfloat16))

        def attend(chunk, carried):
            base = chunk * rows_b
            half = chunk * HALVES // CHUNKS
            half_base = base - half * (n_batch // HALVES)
            wide = pl.BlockSpec((seq, q_width), lambda b, h: (b + base, h))
            wide_in = pl.BlockSpec((seq, q_width), lambda b, h: (b + half_base, h))
            kv_spec = pl.BlockSpec((seq, KV_WIDTH), lambda b, h: (b, h))
            in_specs = [pl.BlockSpec(memory_space=pltpu.SMEM), pl.BlockSpec((seq, table_width), lambda b, h: (b + base, 0)), wide_in, wide_in] + [kv_spec] * 4
            aliases = {}
            if carried:
                in_specs += [pl.BlockSpec(memory_space=pl.ANY)] * 2
                aliases = {8: 0, 9: 1}
            full = jax.ShapeDtypeStruct((tokens, n_kv * q_width), jnp.bfloat16)
            part = jax.ShapeDtypeStruct((chunk_rows, kv_cols), jnp.float32)
            work = rows_b * n_kv * group * seq * 4 * seq
            return pl.pallas_call(
                attend_kernel, grid=(rows_b, n_kv), in_specs=in_specs, out_specs=[wide, wide] + [kv_spec] * 4,
                out_shape=[full, full] + [part] * 4, input_output_aliases=aliases,
                compiler_params=pltpu.CompilerParams(dimension_semantics=('arbitrary', 'arbitrary'), vmem_limit_bytes=48 * 1024 * 1024),
                cost_estimate=pl.CostEstimate(flops=work * HEAD_DIM * 12, bytes_accessed=chunk_rows * (n_kv * q_width * 10 + kv_cols * 24), transcendentals=work),
            )(flags, table, q_half[half], da_half[half], own[chunk], from_a[chunk], from_b[chunk], from_c[chunk], *carried)

        def add(left, right):
            return pl.pallas_call(
                add_kernel, grid=(rows_b,), in_specs=[row_spec(kv_cols)] * 2, out_specs=row_spec(kv_cols),
                out_shape=jax.ShapeDtypeStruct(left.shape, left.dtype), name='add_partial',
                cost_estimate=pl.CostEstimate(flops=chunk_rows * kv_cols * 300, bytes_accessed=chunk_rows * kv_cols * 12, transcendentals=0),
            )(left, right)

        carried = ()
        partials = []
        for c in range(CHUNKS):
            attn, dq_lin, d_own, d_a, d_b, d_c = attend(c, carried)
            carried = (attn, dq_lin)
            back_c = send(d_c, reverse(PAIRS_C))
            back_a = send(d_a, reverse(PAIRS_A))
            back_b = send(add(d_b, back_c), reverse(PAIRS_B))
            partials.append((d_own, back_a, back_b))

        out_proj = jnp.dot(attn, w_o, preferred_element_type=jnp.float32)
        out_tokens = (x_float + out_proj).astype(jnp.bfloat16)
        d_normed_q = jnp.einsum('tf,df->td', dq_lin, w_q, preferred_element_type=jnp.float32)
        d_normed_q = lax.optimization_barrier(d_normed_q)

        dkv_lin = None
        for c, (d_own, back_a, back_b) in enumerate(partials):
            base = c * rows_b
            in_specs = [row_spec(table_width, base)] + [row_spec(kv_cols)] * 3
            operands = [table, d_own, back_a, back_b]
            if dkv_lin is not None:
                in_specs.append(pl.BlockSpec(memory_space=pl.ANY))
                operands.append(dkv_lin)
            dkv_lin = pl.pallas_call(
                finish_kernel, grid=(rows_b,), in_specs=in_specs, out_specs=row_spec(kv_cols, base),
                out_shape=jax.ShapeDtypeStruct((tokens, kv_cols), jnp.bfloat16), input_output_aliases={4: 0} if c else {}, name='finish_kv',
                cost_estimate=pl.CostEstimate(flops=chunk_rows * kv_cols * 300, bytes_accessed=chunk_rows * kv_cols * 14, transcendentals=0),
            )(*operands)

        d_normed = (d_normed_q + jnp.einsum('tf,df->td', dkv_lin, w_kv, preferred_element_type=jnp.float32)).astype(jnp.bfloat16)
        d_gain = jnp.sum(d_normed * x_hat, axis=0)
        d_bias = jnp.sum(d_normed, axis=0, dtype=jnp.float32)
        d_hat = d_normed * (1.0 + ln_gain)
        d_x = inv_std * (d_hat - jnp.mean(d_hat, axis=-1, keepdims=True) - x_hat * jnp.mean(d_hat * x_hat, axis=-1, keepdims=True))
        dx_tokens = (dy_flat.astype(jnp.float32) + d_x).astype(jnp.bfloat16)
        return out_tokens.reshape(x_tokens.shape), dx_tokens.reshape(x_tokens.shape), d_gain, d_bias

    tok_spec = P('dp', 'sp', None)
    rep_vec = P(None)
    rep_mat = P(None, None)
    part_vec = P(('dp', 'sp'))
    return jax.shard_map(block_step, mesh=mesh,
                         in_specs=(tok_spec, tok_spec, P('dp', 'sp'), rep_vec, rep_vec, rep_mat, rep_mat, rep_mat, rep_mat),
                         out_specs=(tok_spec, tok_spec, part_vec, part_vec), check_vma=False)
```
